128 devices in a mesh: dp: 8 (over z, core), sp: 16 (over y, x).
Axes of the slice: x: 4, y: 4, z: 4, core: 2. Of those that a mesh axis runs over, the one named last changes fastest.
Arguments:
- queries_in: bfloat16 [16, 16384, 16, 128], P('dp', 'sp'), may hold values from -6 to 6
- keys_in: bfloat16 [16, 16384, 16, 128], P('dp', 'sp'), may hold values from -6 to 6
- values_in: bfloat16 [16, 16384, 16, 128], P('dp', 'sp'), may hold values from -6 to 6
- out_weight: bfloat16 [2048, 2048], P('dp'), may hold values from -0.125 to 0.125
Outputs:
- block_out: bfloat16 [16, 16384, 2048], P('dp', 'sp')
The draws below stay inside these ranges and needn't reach their ends.
All inputs are finite; a program needn't handle non-finite values.
Results may differ from the reference program's by a relative error of at most 0.006.
Values may be sent and summed in bfloat16 or wider, within the bound.
A program may use at most 320 MiB of HBM per device.

```python
import jax
import jax.numpy as jnp
from jax import lax

HEADS = 16
HEAD_SIZE = 128
BATCH = 16
TOKENS = 16384
WIDTH = 2048


def block_levels(own_key, dims, cuts, least, top_value):
    def one(dim, shards_of):
        draws = jax.random.uniform(jax.random.fold_in(jax.random.fold_in(own_key, 6), dim), (shards_of,), jnp.float32, least / len(cuts), top_value / len(cuts))
        return jnp.repeat(jnp.exp(draws), dims[dim] // shards_of).reshape((-1,) + (1,) * (len(dims) - dim - 1))

    gain = one(*cuts[0])
    for cut in cuts[1:]:
        gain = gain * one(*cut)
    return gain


def bell_draw(key, extent, deviation, limit, cuts=(), kind=jnp.bfloat16):
    loudness = block_levels(key, extent, cuts, -0.22, 0.18) if cuts else 1.0
    drawn = jax.random.normal(key, extent, jnp.float32) * deviation * loudness
    return jnp.minimum(jnp.maximum(drawn, -limit), limit).astype(kind)


def setup_inputs(seed: int = 0) -> dict:
    key_list = jax.random.split(jax.random.key(seed), 5)
    queries_in = bell_draw(key_list[0], (BATCH, TOKENS, HEADS, HEAD_SIZE), 1.0, 6.0, ((0, 8), (1, 16)))
    keys_in = bell_draw(key_list[1], (BATCH, TOKENS, HEADS, HEAD_SIZE), 1.0, 6.0, ((0, 8), (1, 16)))
    values_in = bell_draw(key_list[2], (BATCH, TOKENS, HEADS, HEAD_SIZE), 1.0, 6.0, ((0, 8), (1, 16)))
    out_weight = bell_draw(key_list[3], (WIDTH, WIDTH), WIDTH ** -0.5, 0.125, ((0, 8),))
    return dict(queries_in=queries_in, keys_in=keys_in, values_in=values_in, out_weight=out_weight)


def feature_map(values):
    wide = values.astype(jnp.float32)
    return (wide * wide + 0.1).astype(jnp.bfloat16)


def finish_heads(read, count):
    result = read * count ** 0.5
    return result.astype(jnp.bfloat16)


def look_up(features, state, mass):
    small = lax.optimization_barrier(state.astype(jnp.bfloat16))
    top = jnp.einsum("bthd,bhde->bthe", features.astype(jnp.float32), small.astype(jnp.float32))
    bottom = jnp.einsum("bthd,bhd->bth", features.astype(jnp.float32), mass, precision=lax.Precision.HIGHEST)
    return top / (bottom + 1e-3)[..., None]


def reference(queries_in, keys_in, values_in, out_weight):
    query_feature, key_feature = lax.optimization_barrier((feature_map(queries_in), feature_map(keys_in)))
    state = jnp.einsum("bthd,bthe->bhde", key_feature.astype(jnp.float32), values_in.astype(jnp.float32)) / TOKENS
    mass = jnp.sum(key_feature.astype(jnp.float32), axis=1) / TOKENS
    mixed = finish_heads(look_up(query_feature, state, mass), TOKENS).reshape(BATCH, TOKENS, WIDTH)
    mixed = lax.optimization_barrier(mixed)
    block_out = jnp.einsum("btw,wv->btv", mixed.astype(jnp.float32), out_weight.astype(jnp.float32)).astype(jnp.bfloat16)
    return block_out
```

```python
import functools

import jax
import jax.numpy as jnp
from jax import lax
from jax.experimental import pallas as pl
from jax.experimental.pallas import tpu as pltpu
from jax.sharding import PartitionSpec as P

MESH = pl.DeviceIdType.MESH
F32, BF16 = jnp.float32, jnp.bfloat16
B, T, H, D = 2, 1024, 16, 128
TB = 256
NC = T // TB
ROWS = 272
COUNT = 16384.0


def feature(x):
    wide = x.astype(F32)
    return (wide * wide + 0.1).astype(BF16)


def gather_kernel(
    k_hbm, v_hbm, w_hbm, w_out, st,
    kbuf, vbuf, wv, acc, macc, ps, r1, p2, r2, tmp,
    in_sem, loc_sem, out_sem,
    wz_s, wz_r, wp_s, wp_r, w1_s, w1_r, w2_s, w2_r, wd_s, wd_r,
    s1_s, s1_r, s2_s, s2_r, g1_s, g1_r, g2_s, g2_r,
):
    dp, sp = lax.axis_index("dp"), lax.axis_index("sp")
    z, c = dp // 2, dp % 2
    y, x = sp // 4, sp % 4
    a2, b2 = y * (1 - c) + x * c, x * (1 - c) + y * c

    def plane(dx, dy):
        return (dp, 4 * ((y + dy) % 4) + (x + dx) % 4)

    def along(dz):
        return (2 * ((z + dz) % 4) + c, sp)

    sibling = (2 * z + (1 - c), sp)

    def remote(src, dst, s, r, dev):
        return pltpu.make_async_remote_copy(
            src_ref=src, dst_ref=dst, send_sem=s, recv_sem=r, device_id=dev, device_id_type=MESH
        )

    def load(b, i):
        sl = pl.ds(i * TB, TB)
        n = b * NC + i
        return (
            pltpu.make_async_copy(k_hbm.at[b, sl], kbuf.at[b, sl], in_sem.at[0, n]),
            pltpu.make_async_copy(v_hbm.at[b, sl], vbuf.at[b, sl], in_sem.at[1, n]),
        )

    for b in range(B):
        for i in range(NC):
            for cp in load(b, i):
                cp.start()
    own = 2 * z + c
    keep = pltpu.make_async_copy(w_hbm, wv.at[own], loc_sem)
    keep.start()

    barrier = pltpu.get_barrier_semaphore()
    peers = [along(1), along(2), along(3), sibling]
    peers += [plane(o, 0) for o in (1, 2, 3)] + [plane(0, o) for o in (1, 2, 3)]
    for dev in peers:
        pl.semaphore_signal(barrier, inc=1, device_id=dev, device_id_type=MESH)
    acc[...] = jnp.zeros_like(acc)
    macc[...] = jnp.zeros_like(macc)
    tmp[...] = jnp.zeros_like(tmp)
    pl.semaphore_wait(barrier, len(peers))

    piece = pl.ds((4 * a2 + b2) * 16, 16)

    def far_send():
        return remote(w_hbm.at[piece], wv.at[own, piece], wp_s, wp_r, along(2))

    far = 2 * ((z + 2) % 4) + c

    def near(dz, i):
        k = 0 if dz == 1 else 1
        sl = pl.ds(i * 64, 64)
        return remote(w_hbm.at[sl], wv.at[own, sl], wz_s.at[k, i], wz_r.at[k, i], along(dz))

    def first(o):
        return remote(
            wv.at[far, piece], wv.at[far, piece], w1_s.at[o - 1], w1_r.at[o - 1],
            plane(o * (1 - c), o * c),
        )

    def second(o):
        sl = pl.ds(a2 * 64, 64)
        return remote(
            wv.at[far, sl], wv.at[far, sl], w2_s.at[o - 1], w2_r.at[o - 1],
            plane(o * c, o * (1 - c)),
        )

    def cross(src, dst, n):
        return remote(src, dst, wd_s.at[n], wd_r.at[n], sibling)

    def cross_own():
        return cross(w_hbm, wv.at[own], 0)

    def cross_near(dz, i):
        s = 2 * ((z + dz) % 4) + c
        sl = pl.ds(i * 64, 64)
        return cross(wv.at[s, sl], wv.at[s, sl], 1 + (0 if dz == 1 else 4) + i)

    def cross_far():
        return cross(wv.at[far], wv.at[far], 9)

    far_send().start()
    for i in range(4):
        near(1, i).start()
        near(3, i).start()
    cross_own().start()

    def coords(g):
        return (x, y) if g == 0 else (y, x)

    def ax1(g, o):
        return plane(o, 0) if g == 0 else plane(0, o)

    def ax2(g, o):
        return plane(0, o) if g == 0 else plane(o, 0)

    def rs1(b, g, o):
        a, _ = coords(g)
        n = b * 2 + g
        return remote(
            ps.at[b, g, (a + o) % 4], r1.at[b, g, o - 1], s1_s.at[n, o - 1], s1_r.at[n, o - 1], ax1(g, o)
        )

    def rs2(b, g, o):
        _, l = coords(g)
        n = b * 2 + g
        return remote(
            p2.at[b, g, (l + o) % 4], r2.at[b, g, o - 1], s2_s.at[n, o - 1], s2_r.at[n, o - 1], ax2(g, o)
        )

    def ag1(b, g, o):
        a, l = coords(g)
        n = b * 2 + g
        part = st.at[b, g, a, pl.ds(l * 64, 64)]
        return remote(part, part, g1_s.at[n, o - 1], g1_r.at[n, o - 1], ax2(g, o))

    def ag2(b, g, o):
        a, _ = coords(g)
        n = b * 2 + g
        part = st.at[b, g, a]
        return remote(part, part, g2_s.at[n, o - 1], g2_r.at[n, o - 1], ax1(g, o))

    def mass_block(total):
        hi = total.astype(BF16)
        lo = (total - hi.astype(F32)).astype(BF16)
        tmp[0:2, :] = hi.astype(F32)
        tmp[2:4, :] = lo.astype(F32)
        return tmp[...].astype(BF16)

    def start_rs1(b):
        mass = macc[b]
        for g in range(2):
            for j in range(4):
                h = g * 8 + 2 * j
                ps[b, g, j, 0:128, :] = acc[b, h].astype(BF16)
                ps[b, g, j, 128:256, :] = acc[b, h + 1].astype(BF16)
                ps[b, g, j, 256:272, :] = mass_block(mass[h : h + 2])
        for o in (2, 1, 3):
            for g in range(2):
                rs1(b, g, o).start()

    def start_rs2(b):
        for g in range(2):
            a, l = coords(g)
            for o in (1, 2, 3):
                rs1(b, g, o).wait_recv()
            h = g * 8 + 2 * a
            for half in range(2):
                rows = slice(half * 128, half * 128 + 128)
                total = acc[b, h + half]
                for s in range(3):
                    total = total + r1[b, g, s, rows, :].astype(F32)
                acc[b, h + half] = total
                low = total.astype(BF16)
                p2[b, g, 2 * half, 0:64, :] = low[0:64]
                p2[b, g, 2 * half + 1, 0:64, :] = low[64:128]
            blk = ps[b, g, a, 256:272, :].astype(F32)
            for s in range(3):
                blk = blk + r1[b, g, s, 256:272, :].astype(F32)
            out = mass_block(blk[0:2] + blk[2:4])
            for j in range(4):
                p2[b, g, j, 64:80, :] = out
            for o in (2, 1, 3):
                rs2(b, g, o).start()

    def start_ag1(b):
        for g in range(2):
            a, l = coords(g)
            for o in (1, 2, 3):
                rs2(b, g, o).wait_recv()
            h = g * 8 + 2 * a + l // 2
            total = acc[b, h, pl.ds((l % 2) * 64, 64), :]
            for s in range(3):
                total = total + r2[b, g, s, 0:64, :].astype(F32)
            st[b, g, a, pl.ds(l * 64, 64), :] = (total * (1.0 / COUNT)).astype(BF16)
            blk = p2[b, g, 0, 64:80, :].astype(F32)
            for s in range(3):
                blk = blk + r2[b, g, s, 64:80, :].astype(F32)
            st[b, g, a, 256:272, :] = mass_block((blk[0:2] + blk[2:4]) * (1.0 / COUNT))
            for o in (2, 1, 3):
                ag1(b, g, o).start()

    def start_ag2(b):
        for g in range(2):
            for o in (1, 2, 3):
                ag1(b, g, o).wait_recv()
            for o in (2, 1, 3):
                ag2(b, g, o).start()

    def end_ag2(b):
        for g in range(2):
            for o in (1, 2, 3):
                ag2(b, g, o).wait_recv()

    def start_first():
        remote(wv.at[far, piece], wv.at[far, piece], wp_s, wp_r, along(2)).wait_recv()
        for o in (2, 1, 3):
            first(o).start()

    def start_second():
        for o in (1, 2, 3):
            first(o).wait_recv()
        for o in (2, 1, 3):
            second(o).start()

    def near_arrived(dz, i):
        s = 2 * ((z + dz) % 4) + c
        sl = pl.ds(i * 64, 64)
        k = 1 if dz == 1 else 0
        remote(wv.at[s, sl], wv.at[s, sl], wz_s.at[k, i], wz_r.at[k, i], along(dz)).wait_recv()
        cross_near(dz, i).start()

    def chunk(n, _):
        b, i = n // NC, n % NC
        sl = pl.ds(pl.multiple_of(i * TB, TB), TB)
        for cp in load(b, i):
            cp.wait()
        kf = feature(kbuf[b, sl])
        macc[b] += jnp.sum(kf.astype(F32), axis=0)
        kt = jnp.swapaxes(kf, 0, 1)
        vt = jnp.swapaxes(vbuf[b, sl], 0, 1)
        for h in range(H):
            acc[b, h] += lax.dot_general(
                kt[h], vt[h], (((0,), (0,)), ((), ())), preferred_element_type=F32
            )

        @pl.when(n == 2)
        def _():
            start_first()

        @pl.when(n == 3)
        def _():
            start_rs1(0)

        @pl.when(n == 4)
        def _():
            start_second()

        @pl.when(n == 6)
        def _():
            start_rs2(0)

        @pl.when(n == 7)
        def _():
            start_rs1(1)

        return 0

    lax.fori_loop(0, B * NC, chunk, 0)
    start_ag1(0)
    for dz in (1, 3):
        near_arrived(dz, 0)
        near_arrived(dz, 1)
    start_ag2(0)
    start_rs2(1)
    for o in (1, 2, 3):
        second(o).wait_recv()
    cross_far().start()
    start_ag1(1)
    end_ag2(0)
    start_ag2(1)
    for i in (2, 3):
        for dz in (1, 3):
            near_arrived(dz, i)
    end_ag2(1)

    keep.wait()
    for n in range(10):
        if n == 0:
            s, sl = 2 * z + (1 - c), pl.ds(0, 256)
        elif n == 9:
            s, sl = 2 * ((z + 2) % 4) + (1 - c), pl.ds(0, 256)
        else:
            dz, i = (1, n - 1) if n < 5 else (3, n - 5)
            s, sl = 2 * ((z + dz) % 4) + (1 - c), pl.ds(i * 64, 64)
        cross(wv.at[s, sl], wv.at[s, sl], n).wait_recv()
    done = pltpu.make_async_copy(wv, w_out, out_sem)
    done.start()

    far_send().wait_send()
    for i in range(4):
        near(1, i).wait_send()
        near(3, i).wait_send()
        cross_near(1, i).wait_send()
        cross_near(3, i).wait_send()
    cross_own().wait_send()
    cross_far().wait_send()
    for o in (1, 2, 3):
        first(o).wait_send()
        second(o).wait_send()
        for b in range(B):
            for g in range(2):
                rs1(b, g, o).wait_send()
                rs2(b, g, o).wait_send()
                ag1(b, g, o).wait_send()
                ag2(b, g, o).wait_send()
    done.wait()


def gather(k, v, w):
    dma = pltpu.SemaphoreType.DMA
    return pl.pallas_call(
        gather_kernel,
        out_shape=(
            jax.ShapeDtypeStruct((8, 256, 2048), BF16),
            jax.ShapeDtypeStruct((B, 2, 4, ROWS, D), BF16),
        ),
        in_specs=[pl.BlockSpec(memory_space=pl.ANY)] * 3,
        out_specs=(pl.BlockSpec(memory_space=pl.ANY), pl.BlockSpec(memory_space=pltpu.VMEM)),
        scratch_shapes=[
            pltpu.VMEM((B, T, H, D), BF16),
            pltpu.VMEM((B, T, H, D), BF16),
            pltpu.VMEM((8, 256, 2048), BF16),
            pltpu.VMEM((B, H, D, D), F32),
            pltpu.VMEM((B, H, D), F32),
            pltpu.VMEM((B, 2, 4, ROWS, D), BF16),
            pltpu.VMEM((B, 2, 3, ROWS, D), BF16),
            pltpu.VMEM((B, 2, 4, 80, D), BF16),
            pltpu.VMEM((B, 2, 3, 80, D), BF16),
            pltpu.VMEM((16, D), F32),
            dma((2, B * NC)), dma, dma,
            dma((2, 4)), dma((2, 4)), dma, dma, dma((3,)), dma((3,)), dma((3,)), dma((3,)),
            dma((10,)), dma((10,)),
            dma((4, 3)), dma((4, 3)), dma((4, 3)), dma((4, 3)),
            dma((4, 3)), dma((4, 3)), dma((4, 3)), dma((4, 3)),
        ],
        compiler_params=pltpu.CompilerParams(
            collective_id=0, has_side_effects=True, vmem_limit_bytes=60 * 2**20
        ),
        name="gather",
    )(k, v, w)


def finish_kernel(q_ref, st_ref, w_ref, o_ref, rhs, mixed):
    b = pl.program_id(0)

    @pl.when(pl.program_id(1) == 0)
    def _():
        rhs[...] = jnp.zeros_like(rhs)
        for h in range(H):
            g, j, i = h // 8, (h % 8) // 2, h % 2
            rhs[h, 0:128, 0:128] = st_ref[b, g, j, i * 128 : (i + 1) * 128, :]
            blk = st_ref[b, g, j, 256:272, :].astype(F32)
            hi = jnp.broadcast_to(blk[i : i + 1], (128, 128))
            lo = jnp.broadcast_to(blk[2 + i : 3 + i], (128, 128))
            rhs[h, 0:128, 128:256] = hi.T.astype(BF16)
            rhs[h, 128:256, 128:256] = lo.T.astype(BF16)

    fq = jnp.swapaxes(feature(q_ref[0]), 0, 1)
    for h in range(H):
        r = jnp.dot(
            jnp.concatenate([fq[h], fq[h]], axis=1), rhs[h], preferred_element_type=F32
        )
        read = r[:, 0:128] / (r[:, 128:256] + 0.001)
        mixed[:, h * 128 : (h + 1) * 128] = (read * COUNT**0.5).astype(BF16)
    for n in range(4):
        cols = slice(n * 512, (n + 1) * 512)
        o_ref[0, :, cols] = jnp.dot(
            mixed[...], w_ref[:, cols], preferred_element_type=F32
        ).astype(BF16)


def finish(q, st, w):
    TM = 256
    return pl.pallas_call(
        finish_kernel,
        grid=(B, T // TM),
        in_specs=[
            pl.BlockSpec((1, TM, H, D), lambda b, i: (b, i, 0, 0)),
            pl.BlockSpec((B, 2, 4, ROWS, D), lambda b, i: (0, 0, 0, 0, 0)),
            pl.BlockSpec((2048, 2048), lambda b, i: (0, 0)),
        ],
        out_specs=pl.BlockSpec((1, TM, 2048), lambda b, i: (b, i, 0)),
        out_shape=jax.ShapeDtypeStruct((B, T, 2048), BF16),
        scratch_shapes=[pltpu.VMEM((H, 256, 256), BF16), pltpu.VMEM((TM, 2048), BF16)],
        compiler_params=pltpu.CompilerParams(vmem_limit_bytes=60 * 2**20),
        name="finish",
    )(q, st, w)


def on_device(queries_in, keys_in, values_in, out_weight):
    w, st = gather(keys_in, values_in, out_weight)
    return finish(queries_in, st, w.reshape(2048, 2048))


def solution(mesh):
    placed = (
        P("dp", "sp", None, None),
        P("dp", "sp", None, None),
        P("dp", "sp", None, None),
        P("dp", None),
    )
    return jax.shard_map(
        on_device, mesh=mesh, in_specs=placed, out_specs=P("dp", "sp", None), check_vma=False
    )
```

```python
import functools

import jax
import jax.numpy as jnp
from jax import lax
from jax.experimental import pallas as pl
from jax.experimental.pallas import tpu as pltpu
from jax.sharding import PartitionSpec as P

MESH = pl.DeviceIdType.MESH
F32, BF16 = jnp.float32, jnp.bfloat16
B, T, H, D = 2, 1024, 16, 128
TB = 512
PITCH = 20
STEP = 32
TM = 256
NC = T // TB
ROWS = 272
TN = 512
COUNT = 16384.0


def feature(x):
    wide = x.astype(F32)
    return (wide * wide + 0.1).astype(BF16)


def look_up_columns(st, rhs, cols_of):
    cols_of[...] = jnp.zeros_like(cols_of)
    for g in range(2):
        for j in range(4):
            h = g * 8 + 2 * j
            blk = st[g, j, 256:272, :].astype(F32)
            cols_of[h : h + 2, :] = blk[0:2]
            cols_of[16 + h : 18 + h, :] = blk[2:4]
    mass = cols_of[...].T
    for h in range(H):
        g, j, i = h // 8, (h % 8) // 2, h % 2
        rhs[h, 0:128, 0:128] = st[g, j, i * 128 : (i + 1) * 128, :]
        rhs[h, 128:256, 0:128] = jnp.zeros((128, 128), BF16)
        rhs[h, 0:128, 128:256] = jnp.broadcast_to(mass[:, h : h + 1], (128, 128)).astype(BF16)
        rhs[h, 128:256, 128:256] = jnp.broadcast_to(
            mass[:, 16 + h : 17 + h], (128, 128)
        ).astype(BF16)


def look_up(fq, rhs, mixed, lo, hi):
    def step(h, _):
        for t in range(T // TM):
            rows = slice(t * TM, (t + 1) * TM)
            f = fq[h, rows, :]
            r = jnp.dot(jnp.concatenate([f, f], axis=1), rhs[h], preferred_element_type=F32)
            read = r[:, 0:128] / (r[:, 128:256] + 0.001)
            mixed[rows, pl.ds(pl.multiple_of(h * D, D), D)] = (read * COUNT**0.5).astype(BF16)
        return 0

    lax.fori_loop(lo, hi, step, 0, unroll=4)


def gather_kernel(
    q_hbm, k_hbm, v_hbm, w_hbm, w_out, out0, fq1, st1,
    kbuf, vbuf, kf32, vf32, wv, acc, macc, ps, r1, xs, xr, st, tmp, fq, mixed, rhs, cols_of, obuf,
    in_sem, q_sem, loc_sem, out_sem, w_sem, m_sem,
    wz_s, wz_r, wp_s, wp_r, w1_s, w1_r, w2_s, w2_r, wd_s, wd_r,
    s1_s, s1_r, s2_s, s2_r, s3_s, s3_r,
):
    dp, sp = lax.axis_index("dp"), lax.axis_index("sp")
    z, c = dp // 2, dp % 2
    y, x = sp // 4, sp % 4
    a2, b2 = y * (1 - c) + x * c, x * (1 - c) + y * c

    def plane(dx, dy):
        return (dp, 4 * ((y + dy) % 4) + (x + dx) % 4)

    def along(dz):
        return (2 * ((z + dz) % 4) + c, sp)

    sibling = (2 * z + (1 - c), sp)

    def remote(src, dst, s, r, dev):
        return pltpu.make_async_remote_copy(
            src_ref=src, dst_ref=dst, send_sem=s, recv_sem=r, device_id=dev, device_id_type=MESH
        )

    def load(b, i):
        sl = pl.ds(i * TB, TB)
        n = b * NC + i
        return (
            pltpu.make_async_copy(k_hbm.at[b, sl], kbuf.at[b, sl], in_sem.at[0, n]),
            pltpu.make_async_copy(v_hbm.at[b, sl], vbuf.at[b, sl], in_sem.at[1, n]),
        )

    def load_q(b):
        return pltpu.make_async_copy(q_hbm.at[b], (kbuf, vbuf)[b].at[0], q_sem.at[b])

    for b in range(B):
        for i in range(NC):
            for cp in load(b, i):
                cp.start()
    own = 2 * z + c

    def shard(s):
        return pl.ds(pl.multiple_of(s * 256, 256), 256)

    keep = pltpu.make_async_copy(w_hbm, wv.at[shard(own)], loc_sem)
    keep.start()

    barrier = pltpu.get_barrier_semaphore()
    peers = [along(1), along(2), along(3), sibling]
    peers += [plane(o, 0) for o in (1, 2, 3)] + [plane(0, o) for o in (1, 2, 3)]
    for dev in peers:
        pl.semaphore_signal(barrier, inc=1, device_id=dev, device_id_type=MESH)
    acc[...] = jnp.zeros_like(acc)
    macc[...] = jnp.zeros_like(macc)
    tmp[...] = jnp.zeros_like(tmp)
    pl.semaphore_wait(barrier, len(peers))

    def far_rows(s, first, count):
        return pl.ds(pl.multiple_of(s * 256 + first * 16, 16), count * 16)

    far = 2 * ((z + 2) % 4) + c
    piece = 4 * a2 + b2

    def far_send():
        return remote(
            w_hbm.at[pl.ds(pl.multiple_of(piece * 16, 16), 16)], wv.at[far_rows(own, piece, 1)],
            wp_s, wp_r, along(2),
        )

    def near(dz, i):
        k = 0 if dz == 1 else 1
        cols = pl.ds(i * TN, TN)
        return remote(
            w_hbm.at[:, cols], wv.at[shard(own), cols], wz_s.at[k, i], wz_r.at[k, i], along(dz)
        )

    def first(o):
        part = wv.at[far_rows(far, piece, 1)]
        return remote(part, part, w1_s.at[o - 1], w1_r.at[o - 1], plane(o * (1 - c), o * c))

    def second(o):
        part = wv.at[far_rows(far, 4 * a2, 4)]
        return remote(part, part, w2_s.at[o - 1], w2_r.at[o - 1], plane(o * c, o * (1 - c)))

    def cross(src, dst, n):
        return remote(src, dst, wd_s.at[n], wd_r.at[n], sibling)

    def cross_own():
        return cross(w_hbm, wv.at[shard(own)], 0)

    def cross_near(dz, i):
        part = wv.at[shard(2 * ((z + dz) % 4) + c), pl.ds(i * TN, TN)]
        return cross(part, part, 1 + (0 if dz == 1 else 4) + i)

    def cross_far():
        part = wv.at[shard(far)]
        return cross(part, part, 9)

    far_send().start()
    for i in range(4):
        near(1, i).start()
        near(3, i).start()
    cross_own().start()

    def place(g):
        return x if g == 0 else y

    def ax1(g, o):
        return plane(o, 0) if g == 0 else plane(0, o)

    def ax2(g, o):
        return plane(0, o) if g == 0 else plane(o, 0)

    def scatter(b, g, o):
        n = b * 2 + g
        return remote(
            ps.at[b, g, (place(g) + o) % 4], r1.at[b, g, o - 1],
            s1_s.at[n, o - 1], s1_r.at[n, o - 1], ax1(g, o),
        )

    def exchange(b, g, o):
        n = b * 2 + g
        return remote(
            xs.at[b, g], xr.at[b, g, o - 1], s2_s.at[n, o - 1], s2_r.at[n, o - 1], ax2(g, o)
        )

    def spread(b, g, o):
        n = b * 2 + g
        part = st.at[b, g, place(g)]
        return remote(part, part, s3_s.at[n, o - 1], s3_r.at[n, o - 1], ax1(g, o))

    def mass_block(total):
        hi = total.astype(BF16)
        lo = (total - hi.astype(F32)).astype(BF16)
        tmp[0:2, :] = hi.astype(F32)
        tmp[2:4, :] = lo.astype(F32)
        return tmp[...].astype(BF16)

    def start_scatter(b):
        mass = macc[b]
        for g in range(2):
            for j in range(4):
                h = g * 8 + 2 * j
                ps[b, g, j, 0:128, :] = acc[b, h].astype(BF16)
                ps[b, g, j, 128:256, :] = acc[b, h + 1].astype(BF16)
                ps[b, g, j, 256:272, :] = mass_block(mass[h : h + 2])
        for o in (2, 1, 3):
            for g in range(2):
                scatter(b, g, o).start()

    def start_exchange(b):
        for g in range(2):
            a = place(g)
            for o in (1, 3, 2):
                scatter(b, g, o).wait_recv()
            h = g * 8 + 2 * a
            for i in range(2):
                rows = slice(i * 128, i * 128 + 128)
                total = acc[b, h + i]
                for s in range(3):
                    total = total + r1[b, g, s, rows, :].astype(F32)
                acc[b, h + i] = total
                xs[b, g, rows, :] = total.astype(BF16)
            blk = ps[b, g, a, 256:272, :].astype(F32)
            for s in range(3):
                blk = blk + r1[b, g, s, 256:272, :].astype(F32)
            xs[b, g, 256:272, :] = mass_block(blk[0:2] + blk[2:4])
            for o in (2, 1, 3):
                exchange(b, g, o).start()

    def start_spread(b):
        for g in range(2):
            a = place(g)
            for o in (1, 3, 2):
                exchange(b, g, o).wait_recv()
            h = g * 8 + 2 * a
            for i in range(2):
                rows = slice(i * 128, i * 128 + 128)
                total = acc[b, h + i]
                for s in range(3):
                    total = total + xr[b, g, s, rows, :].astype(F32)
                st[b, g, a, rows, :] = (total * (1.0 / COUNT)).astype(BF16)
            blk = xs[b, g, 256:272, :].astype(F32)
            for s in range(3):
                blk = blk + xr[b, g, s, 256:272, :].astype(F32)
            st[b, g, a, 256:272, :] = mass_block((blk[0:2] + blk[2:4]) * (1.0 / COUNT))
            for o in (2, 1, 3):
                spread(b, g, o).start()

    def end_spread(b):
        for g in range(2):
            for o in (1, 3, 2):
                spread(b, g, o).wait_recv()

    def start_first():
        part = wv.at[far_rows(far, piece, 1)]
        remote(part, part, wp_s, wp_r, along(2)).wait_recv()
        for o in (2, 1, 3):
            first(o).start()

    def start_second():
        for o in (1, 3, 2):
            first(o).wait_recv()
        for o in (2, 1, 3):
            second(o).start()

    def start_cross_far():
        for o in (1, 3, 2):
            second(o).wait_recv()
        cross_far().start()

    def start_cross_near(i):
        for dz in (1, 3):
            part = wv.at[shard(2 * ((z + dz) % 4) + c), pl.ds(i * TN, TN)]
            k = 1 if dz == 1 else 0
            remote(part, part, wz_s.at[k, i], wz_r.at[k, i], along(dz)).wait_recv()
            cross_near(dz, i).start()

    def wait_cross(n):
        if n == 0:
            part = wv.at[shard(2 * z + (1 - c))]
        elif n == 9:
            part = wv.at[shard(2 * ((z + 2) % 4) + (1 - c))]
        else:
            dz, i = (1, n - 1) if n < 5 else (3, n - 5)
            part = wv.at[shard(2 * ((z + dz) % 4) + (1 - c)), pl.ds(i * TN, TN)]
        cross(part, part, n).wait_recv()

    def chunk(n, _):
        b, i = n // NC, n % NC
        sl = pl.ds(pl.multiple_of(i * TB, TB), TB)
        for cp in load(b, i):
            cp.wait()

        def fill(j, mass):
            rows = []
            for t in range(STEP):
                at = i * TB + j * STEP + t
                f = feature(kbuf[b, at]).astype(F32)
                kf32[pl.ds((j * STEP + t) * PITCH, H), :] = f
                vf32[pl.ds((j * STEP + t) * PITCH, H), :] = vbuf[b, at].astype(F32)
                rows.append(f)
            while len(rows) > 1:
                rows = [p + q for p, q in zip(rows[::2], rows[1::2])]
            return mass + rows[0]

        macc[b] += lax.fori_loop(0, TB // STEP, fill, jnp.zeros((H, D), F32))
        for h in range(H):
            kh = kf32[pl.ds(h, TB, stride=PITCH), :].astype(BF16)
            vh = vf32[pl.ds(h, TB, stride=PITCH), :].astype(BF16)
            acc[b, h] += lax.dot_general(
                kh, vh, (((0,), (0,)), ((), ())), preferred_element_type=F32
            )

        @pl.when(n == 0)
        def _():
            start_first()

        @pl.when(n == NC - 1)
        def _():
            start_scatter(0)
            for b in range(B):
                load_q(b).start()

        return 0

    lax.fori_loop(0, B * NC, chunk, 0)
    start_second()
    start_exchange(0)
    start_scatter(1)
    start_cross_near(0)

    def turn(b):
        load_q(b).wait()

        q = (kbuf, vbuf)[b]

        def step(i, _):
            sl = pl.ds(pl.multiple_of(i * TM, TM), TM)
            fq[b, :, sl, :] = jnp.swapaxes(feature(q[0, sl]), 0, 1)
            return 0

        lax.fori_loop(0, T // TM, step, 0)

    turn(0)
    turn(1)
    put_fq = pltpu.make_async_copy(fq.at[1], fq1, m_sem.at[0])
    put_fq.start()
    start_spread(0)
    start_cross_far()
    start_exchange(1)
    start_cross_near(1)
    def put_out(n):
        return pltpu.make_async_copy(
            obuf.at[n % 2], out0.at[:, pl.ds(n * TN, TN)], out_sem.at[n]
        )

    def put_w(n):
        cols = pl.ds(n * TN, TN)
        return pltpu.make_async_copy(wv.at[:, cols], w_out.at[:, cols], w_sem.at[n])

    end_spread(0)
    look_up_columns(st.at[0], rhs, cols_of)
    look_up(fq.at[0], rhs, mixed, 0, H)
    start_cross_near(2)
    start_spread(1)
    keep.wait()
    wait_cross(0)
    wait_cross(9)
    for n in range(4):
        if n == 1:
            start_cross_near(3)
        if n == 3:
            end_spread(1)
            put_st = pltpu.make_async_copy(st.at[1], st1, m_sem.at[1])
            put_st.start()
        wait_cross(1 + n)
        wait_cross(5 + n)
        if n >= 2:
            put_out(n - 2).wait()
        cols = slice(n * TN, (n + 1) * TN)
        obuf[n % 2] = jnp.dot(mixed[...], wv[:, cols], preferred_element_type=F32).astype(BF16)
        put_out(n).start()
        put_w(n).start()

    far_send().wait_send()
    for i in range(4):
        near(1, i).wait_send()
        near(3, i).wait_send()
        cross_near(1, i).wait_send()
        cross_near(3, i).wait_send()
    cross_own().wait_send()
    cross_far().wait_send()
    for o in (1, 2, 3):
        first(o).wait_send()
        second(o).wait_send()
        for b in range(B):
            for g in range(2):
                scatter(b, g, o).wait_send()
                exchange(b, g, o).wait_send()
                spread(b, g, o).wait_send()
    for n in range(4):
        put_w(n).wait()
    put_out(2).wait()
    put_out(3).wait()
    put_fq.wait()
    put_st.wait()


def gather(q, k, v, w):
    dma = pltpu.SemaphoreType.DMA
    hbm = pl.BlockSpec(memory_space=pl.ANY)
    return pl.pallas_call(
        gather_kernel,
        out_shape=(
            jax.ShapeDtypeStruct((2048, 2048), BF16),
            jax.ShapeDtypeStruct((T, 2048), BF16),
            jax.ShapeDtypeStruct((H, T, D), BF16),
            jax.ShapeDtypeStruct((2, 4, ROWS, D), BF16),
        ),
        in_specs=[hbm] * 4,
        out_specs=(hbm,) * 4,
        scratch_shapes=[
            pltpu.VMEM((B, T, H, D), BF16),
            pltpu.VMEM((B, T, H, D), BF16),
            pltpu.VMEM((TB * PITCH, D), F32),
            pltpu.VMEM((TB * PITCH, D), F32),
            pltpu.VMEM((2048, 2048), BF16),
            pltpu.VMEM((B, H, D, D), F32),
            pltpu.VMEM((B, H, D), F32),
            pltpu.VMEM((B, 2, 4, ROWS, D), BF16),
            pltpu.VMEM((B, 2, 3, ROWS, D), BF16),
            pltpu.VMEM((B, 2, ROWS, D), BF16),
            pltpu.VMEM((B, 2, 3, ROWS, D), BF16),
            pltpu.VMEM((B, 2, 4, ROWS, D), BF16),
            pltpu.VMEM((16, D), F32),
            pltpu.VMEM((B, H, T, D), BF16),
            pltpu.VMEM((T, 2048), BF16),
            pltpu.VMEM((H, 256, 256), BF16),
            pltpu.VMEM((D, D), F32),
            pltpu.VMEM((2, T, TN), BF16),
            dma((2, B * NC)), dma((B,)), dma, dma((4,)), dma((4,)), dma((2,)),
            dma((2, 4)), dma((2, 4)), dma, dma, dma((3,)), dma((3,)), dma((3,)), dma((3,)),
            dma((10,)), dma((10,)),
            dma((4, 3)), dma((4, 3)), dma((4, 3)), dma((4, 3)), dma((4, 3)), dma((4, 3)),
        ],
        compiler_params=pltpu.CompilerParams(
            collective_id=0, has_side_effects=True, vmem_limit_bytes=63 * 2**20
        ),
        name="gather",
    )(q, k, v, w)


def finish_kernel(
    fq_hbm, st_ref, w_hbm, first_hbm, o_hbm,
    fq, rhs, cols_of, mixed, wbuf, fbuf, obuf, q_sem, w_sem, f_sem, o_sem,
):
    def get_q(n):
        hs = pl.ds(n * 4, 4)
        return pltpu.make_async_copy(fq_hbm.at[hs], fq.at[hs], q_sem.at[n])

    def get_w(n):
        cols = pl.ds(n * TN, TN)
        return pltpu.make_async_copy(w_hbm.at[:, cols], wbuf.at[:, cols], w_sem.at[n])

    def put(n):
        return pltpu.make_async_copy(
            obuf.at[n % 2], o_hbm.at[1, :, pl.ds(n * TN, TN)], o_sem.at[n]
        )

    for n in range(4):
        get_q(n).start()
    for n in range(4):
        get_w(n).start()
    get_first = pltpu.make_async_copy(first_hbm, fbuf, f_sem.at[0])
    get_first.start()
    put_first = pltpu.make_async_copy(fbuf, o_hbm.at[0], f_sem.at[1])
    look_up_columns(st_ref, rhs, cols_of)
    for n in range(4):
        get_q(n).wait()
    look_up(fq, rhs, mixed, 0, H)
    for n in range(4):
        get_w(n).wait()
        if n == 0:
            get_first.wait()
            put_first.start()
        if n >= 2:
            put(n - 2).wait()
        cols = slice(n * TN, (n + 1) * TN)
        obuf[n % 2] = jnp.dot(mixed[...], wbuf[:, cols], preferred_element_type=F32).astype(BF16)
        put(n).start()
    put_first.wait()
    put(2).wait()
    put(3).wait()


def finish(fq1, st1, w, out0):
    dma = pltpu.SemaphoreType.DMA
    hbm = pl.BlockSpec(memory_space=pl.ANY)
    return pl.pallas_call(
        finish_kernel,
        in_specs=[hbm, pl.BlockSpec(memory_space=pltpu.VMEM), hbm, hbm],
        out_specs=hbm,
        out_shape=jax.ShapeDtypeStruct((B, T, 2048), BF16),
        scratch_shapes=[
            pltpu.VMEM((H, T, D), BF16),
            pltpu.VMEM((H, 256, 256), BF16),
            pltpu.VMEM((D, D), F32),
            pltpu.VMEM((T, 2048), BF16),
            pltpu.VMEM((2048, 2048), BF16),
            pltpu.VMEM((T, 2048), BF16),
            pltpu.VMEM((2, T, TN), BF16),
            dma((4,)), dma((4,)), dma((2,)), dma((4,)),
        ],
        compiler_params=pltpu.CompilerParams(vmem_limit_bytes=60 * 2**20),
        name="finish",
    )(fq1, st1, w, out0)


def on_device(queries_in, keys_in, values_in, out_weight):
    w, out0, fq1, st1 = gather(queries_in, keys_in, values_in, out_weight)
    return finish(fq1, st1, w, out0)


def solution(mesh):
    placed = (
        P("dp", "sp", None, None),
        P("dp", "sp", None, None),
        P("dp", "sp", None, None),
        P("dp", None),
    )
    return jax.shard_map(
        on_device, mesh=mesh, in_specs=placed, out_specs=P("dp", "sp", None), check_vma=False
    )
```

```python
import functools

import jax
import jax.numpy as jnp
from jax import lax
from jax.experimental import pallas as pl
from jax.experimental.pallas import tpu as pltpu
from jax.sharding import PartitionSpec as P

MESH = pl.DeviceIdType.MESH
F32, BF16 = jnp.float32, jnp.bfloat16
B, T, H, D = 2, 1024, 16, 128
TB = 512
HB = 256
PITCH = 20
STEP = 32
TM = 256
NC = T // TB
ROWS = 272
TN = 512
CN = 1024
COUNT = 16384.0


def feature(x):
    wide = x.astype(F32)
    return (wide * wide + 0.1).astype(BF16)


def look_up(fq, st, rhs, cols_of, mixed, owners):
    heads = []
    for g in range(2):
        j = owners[g]
        blk = st[g, j, 256:272, :].astype(F32)
        cols_of[4 * g : 4 * g + 4, :] = blk[0:4]
        heads += [(g, j, 0), (g, j, 1)]
    mass = cols_of[...].T
    for n, (g, j, i) in enumerate(heads):
        hi, lo = 4 * g + i, 4 * g + 2 + i
        rhs[n, 0:128, 0:128] = st[g, j, i * 128 : (i + 1) * 128, :]
        rhs[n, 0:128, 128:256] = jnp.broadcast_to(mass[:, hi : hi + 1], (128, 128)).astype(BF16)
        rhs[n, 128:256, 128:256] = jnp.broadcast_to(mass[:, lo : lo + 1], (128, 128)).astype(BF16)
    for n, (g, j, i) in enumerate(heads):
        h = g * 8 + 2 * j + i
        for t in range(T // TM):
            rows = slice(t * TM, (t + 1) * TM)
            f = fq[h, rows, :]
            r = jnp.dot(jnp.concatenate([f, f], axis=1), rhs[n], preferred_element_type=F32)
            read = r[:, 0:128] / (r[:, 128:256] + 0.001)
            mixed[rows, pl.ds(pl.multiple_of(h * D, D), D)] = (read * COUNT**0.5).astype(BF16)


def gather_kernel(
    q_hbm, k_hbm, v_hbm, w_hbm, w_out, out0, fq1, st1,
    kbuf, vbuf, kf32, vf32, wv, acc, macc, ps, r1, xs, xr, st, tmp, fq, mixed, rhs, cols_of, obuf,
    in_sem, q_sem, loc_sem, out_sem, w_sem, m_sem,
    wz_s, wz_r, wp_s, wp_r, w1_s, w1_r, w2_s, w2_r, wd_s, wd_r,
    s1_s, s1_r, s2_s, s2_r, s3_s, s3_r,
):
    dp, sp = lax.axis_index("dp"), lax.axis_index("sp")
    z, c = dp // 2, dp % 2
    y, x = sp // 4, sp % 4
    a2, b2 = y * (1 - c) + x * c, x * (1 - c) + y * c

    def plane(dx, dy):
        return (dp, 4 * ((y + dy) % 4) + (x + dx) % 4)

    def along(dz):
        return (2 * ((z + dz) % 4) + c, sp)

    sibling = (2 * z + (1 - c), sp)

    def remote(src, dst, s, r, dev):
        return pltpu.make_async_remote_copy(
            src_ref=src, dst_ref=dst, send_sem=s, recv_sem=r, device_id=dev, device_id_type=MESH
        )

    def load(b, i, half):
        sl = pl.ds(i * TB + half * HB, HB)
        n = 2 * (b * NC + i) + half
        return (
            pltpu.make_async_copy(k_hbm.at[b, sl], kbuf.at[b, sl], in_sem.at[0, n]),
            pltpu.make_async_copy(v_hbm.at[b, sl], vbuf.at[b, sl], in_sem.at[1, n]),
        )

    def start_load(b, i):
        for half in range(2):
            for cp in load(b, i, half):
                cp.start()

    def load_q(b):
        return pltpu.make_async_copy(q_hbm.at[b], (kbuf, vbuf)[b].at[0], q_sem.at[b])

    start_load(0, 0)
    own = 2 * z + c

    def shard(s):
        return pl.ds(pl.multiple_of(s * 256, 256), 256)

    keep = pltpu.make_async_copy(w_hbm, wv.at[shard(own)], loc_sem)

    barrier = pltpu.get_barrier_semaphore()
    peers = [along(1), along(2), along(3), sibling]
    peers += [plane(o, 0) for o in (1, 2, 3)] + [plane(0, o) for o in (1, 2, 3)]
    for dev in peers:
        pl.semaphore_signal(barrier, inc=1, device_id=dev, device_id_type=MESH)
    acc[...] = jnp.zeros_like(acc)
    macc[...] = jnp.zeros_like(macc)
    tmp[...] = jnp.zeros_like(tmp)
    cols_of[...] = jnp.zeros_like(cols_of)
    rhs[...] = jnp.zeros_like(rhs)
    pl.semaphore_wait(barrier, len(peers))

    def far_rows(s, first, count):
        return pl.ds(pl.multiple_of(s * 256 + first * 16, 16), count * 16)

    far = 2 * ((z + 2) % 4) + c
    piece = 4 * a2 + b2

    def far_send():
        return remote(
            w_hbm.at[pl.ds(pl.multiple_of(piece * 16, 16), 16)], wv.at[far_rows(own, piece, 1)],
            wp_s, wp_r, along(2),
        )

    def near(dz, i):
        k = 0 if dz == 1 else 1
        cols = pl.ds(i * TN, TN)
        return remote(
            w_hbm.at[:, cols], wv.at[shard(own), cols], wz_s.at[k, i], wz_r.at[k, i], along(dz)
        )

    def first(o):
        part = wv.at[far_rows(far, piece, 1)]
        return remote(part, part, w1_s.at[o - 1], w1_r.at[o - 1], plane(o * (1 - c), o * c))

    def second(o, i):
        part = wv.at[far_rows(far, 4 * a2, 4), pl.ds(i * CN, CN)]
        return remote(
            part, part, w2_s.at[i, o - 1], w2_r.at[i, o - 1], plane(o * c, o * (1 - c))
        )

    def cross(src, dst, n):
        return remote(src, dst, wd_s.at[n], wd_r.at[n], sibling)

    def cross_own():
        return cross(w_hbm, wv.at[shard(own)], 0)

    def cross_near(dz, i):
        part = wv.at[shard(2 * ((z + dz) % 4) + c), pl.ds(i * TN, TN)]
        return cross(part, part, 1 + (0 if dz == 1 else 4) + i)

    def cross_far(i):
        part = wv.at[shard(far), pl.ds(i * CN, CN)]
        return cross(part, part, 9 + i)

    far_send().start()
    for i in range(4):
        near(1, i).start()
        near(3, i).start()
    cross_own().start()
    start_load(0, 1)

    def place(g):
        return x if g == 0 else y

    def ax1(g, o):
        return plane(o, 0) if g == 0 else plane(0, o)

    def ax2(g, o):
        return plane(0, o) if g == 0 else plane(o, 0)

    def scatter(b, g, o):
        n = b * 2 + g
        return remote(
            ps.at[b, g, (place(g) + o) % 4], r1.at[b, g, o - 1],
            s1_s.at[n, o - 1], s1_r.at[n, o - 1], ax1(g, o),
        )

    def exchange(b, g, o):
        n = b * 2 + g
        return remote(
            xs.at[b, g], xr.at[b, g, o - 1], s2_s.at[n, o - 1], s2_r.at[n, o - 1], ax2(g, o)
        )

    def spread(b, g, o):
        n = b * 2 + g
        part = st.at[b, g, place(g)]
        return remote(part, part, s3_s.at[n, o - 1], s3_r.at[n, o - 1], ax1(g, o))

    def mass_block(total):
        hi = total.astype(BF16)
        lo = (total - hi.astype(F32)).astype(BF16)
        tmp[0:2, :] = hi.astype(F32)
        tmp[2:4, :] = lo.astype(F32)
        return tmp[...].astype(BF16)

    def start_scatter(b):
        mass = macc[b]
        for g in range(2):
            for j in range(4):
                h = g * 8 + 2 * j
                ps[b, g, j, 0:128, :] = acc[b, h].astype(BF16)
                ps[b, g, j, 128:256, :] = acc[b, h + 1].astype(BF16)
                ps[b, g, j, 256:272, :] = mass_block(mass[h : h + 2])
        for o in (2, 1, 3):
            for g in range(2):
                scatter(b, g, o).start()

    def start_exchange(b):
        for g in range(2):
            a = place(g)
            for o in (1, 3, 2):
                scatter(b, g, o).wait_recv()
            h = g * 8 + 2 * a
            for i in range(2):
                rows = slice(i * 128, i * 128 + 128)
                total = acc[b, h + i]
                for s in range(3):
                    total = total + r1[b, g, s, rows, :].astype(F32)
                acc[b, h + i] = total
                xs[b, g, rows, :] = total.astype(BF16)
            blk = ps[b, g, a, 256:272, :].astype(F32)
            for s in range(3):
                blk = blk + r1[b, g, s, 256:272, :].astype(F32)
            xs[b, g, 256:272, :] = mass_block(blk[0:2] + blk[2:4])
            for o in (2, 1, 3):
                exchange(b, g, o).start()

    def start_spread(b):
        for g in range(2):
            a = place(g)
            for o in (1, 3, 2):
                exchange(b, g, o).wait_recv()
            h = g * 8 + 2 * a
            for i in range(2):
                rows = slice(i * 128, i * 128 + 128)
                total = acc[b, h + i]
                for s in range(3):
                    total = total + xr[b, g, s, rows, :].astype(F32)
                st[b, g, a, rows, :] = (total * (1.0 / COUNT)).astype(BF16)
            blk = xs[b, g, 256:272, :].astype(F32)
            for s in range(3):
                blk = blk + xr[b, g, s, 256:272, :].astype(F32)
            st[b, g, a, 256:272, :] = mass_block((blk[0:2] + blk[2:4]) * (1.0 / COUNT))
            for o in (2, 1, 3):
                spread(b, g, o).start()

    def end_spread(b):
        for g in range(2):
            for o in (1, 3, 2):
                spread(b, g, o).wait_recv()

    def start_first():
        part = wv.at[far_rows(far, piece, 1)]
        remote(part, part, wp_s, wp_r, along(2)).wait_recv()
        for o in (2, 1, 3):
            first(o).start()

    def start_second(i):
        if i == 0:
            for o in (1, 3, 2):
                first(o).wait_recv()
        for o in (2, 1, 3):
            second(o, i).start()

    def start_cross_far(i):
        for o in (1, 3, 2):
            second(o, i).wait_recv()
        cross_far(i).start()

    def start_cross_near(i):
        for dz in (1, 3):
            part = wv.at[shard(2 * ((z + dz) % 4) + c), pl.ds(i * TN, TN)]
            k = 1 if dz == 1 else 0
            remote(part, part, wz_s.at[k, i], wz_r.at[k, i], along(dz)).wait_recv()
            cross_near(dz, i).start()

    def wait_cross(n):
        if n == 0:
            part = wv.at[shard(2 * z + (1 - c))]
        elif n >= 9:
            part = wv.at[shard(2 * ((z + 2) % 4) + (1 - c)), pl.ds((n - 9) * CN, CN)]
        else:
            dz, i = (1, n - 1) if n < 5 else (3, n - 5)
            part = wv.at[shard(2 * ((z + dz) % 4) + (1 - c)), pl.ds(i * TN, TN)]
        cross(part, part, n).wait_recv()

    def chunk(n, _):
        b, i = n // NC, n % NC
        @pl.when(n + 2 < B * NC)
        def _():
            start_load((n + 2) // NC, (n + 2) % NC)

        def fill(j, mass):
            rows = []
            for t in range(STEP):
                at = i * TB + j * STEP + t
                f = feature(kbuf[b, at]).astype(F32)
                kf32[pl.ds((j * STEP + t) * PITCH, H), :] = f
                vf32[pl.ds((j * STEP + t) * PITCH, H), :] = vbuf[b, at].astype(F32)
                rows.append(f)
            while len(rows) > 1:
                rows = [p + q for p, q in zip(rows[::2], rows[1::2])]
            return mass + rows[0]

        mass = jnp.zeros((H, D), F32)
        for half in range(2):
            for cp in load(b, i, half):
                cp.wait()
            mass = lax.fori_loop(half * (HB // STEP), (half + 1) * (HB // STEP), fill, mass)
        macc[b] += mass
        for h in range(H):
            kh = kf32[pl.ds(h, TB, stride=PITCH), :].astype(BF16)
            vh = vf32[pl.ds(h, TB, stride=PITCH), :].astype(BF16)
            acc[b, h] += lax.dot_general(
                kh, vh, (((0,), (0,)), ((), ())), preferred_element_type=F32
            )

        @pl.when(n == 0)
        def _():
            start_first()

        @pl.when(n == NC - 1)
        def _():
            start_scatter(0)
            keep.start()
            for b in range(B):
                load_q(b).start()

        return 0

    lax.fori_loop(0, B * NC, chunk, 0)
    start_exchange(0)
    start_second(0)
    start_scatter(1)
    start_cross_near(0)

    def turn(b):
        load_q(b).wait()

        q = (kbuf, vbuf)[b]

        def step(i, _):
            sl = pl.ds(pl.multiple_of(i * TM, TM), TM)
            fq[b, :, sl, :] = jnp.swapaxes(feature(q[0, sl]), 0, 1)
            return 0

        lax.fori_loop(0, T // TM, step, 0)

    turn(0)
    turn(1)
    put_fq = pltpu.make_async_copy(fq.at[1], fq1, m_sem.at[0])
    put_fq.start()
    start_spread(0)
    start_second(1)
    def put_out(n):
        cols = pl.ds(n * TN, TN)
        return pltpu.make_async_copy(obuf.at[:, cols], out0.at[:, cols], out_sem.at[n])

    def put_w(n):
        cols = pl.ds(n * TN, TN)
        return pltpu.make_async_copy(wv.at[:, cols], w_out.at[:, cols], w_sem.at[n])

    for o in (0, 1, 3, 2):
        if o == 1:
            start_cross_near(1)
            start_exchange(1)
            start_cross_far(0)
        if o:
            for g in range(2):
                spread(0, g, o).wait_recv()
        owners = [(place(g) + 4 - o) % 4 for g in range(2)]
        look_up(fq.at[0], st.at[0], rhs, cols_of, mixed, owners)
    start_spread(1)
    start_cross_near(2)
    start_cross_far(1)
    keep.wait()
    wait_cross(0)
    wait_cross(9)
    for n in range(4):
        if n == 1:
            start_cross_near(3)
        if n == 2:
            wait_cross(10)
        if n == 3:
            end_spread(1)
            put_st = pltpu.make_async_copy(st.at[1], st1, m_sem.at[1])
            put_st.start()
        wait_cross(1 + n)
        wait_cross(5 + n)
        cols = slice(n * TN, (n + 1) * TN)
        put_w(n).start()
        obuf[:, cols] = jnp.dot(mixed[...], wv[:, cols], preferred_element_type=F32).astype(BF16)
        put_out(n).start()

    far_send().wait_send()
    for i in range(4):
        near(1, i).wait_send()
        near(3, i).wait_send()
        cross_near(1, i).wait_send()
        cross_near(3, i).wait_send()
    cross_own().wait_send()
    for i in range(2):
        cross_far(i).wait_send()
    for o in (1, 2, 3):
        first(o).wait_send()
        for i in range(2):
            second(o, i).wait_send()
        for b in range(B):
            for g in range(2):
                scatter(b, g, o).wait_send()
                exchange(b, g, o).wait_send()
                spread(b, g, o).wait_send()
    for n in range(4):
        put_w(n).wait()
        put_out(n).wait()
    put_fq.wait()
    put_st.wait()


def gather(q, k, v, w):
    dma = pltpu.SemaphoreType.DMA
    hbm = pl.BlockSpec(memory_space=pl.ANY)
    return pl.pallas_call(
        gather_kernel,
        out_shape=(
            jax.ShapeDtypeStruct((2048, 2048), BF16),
            jax.ShapeDtypeStruct((T, 2048), BF16),
            jax.ShapeDtypeStruct((H, T, D), BF16),
            jax.ShapeDtypeStruct((2, 4, ROWS, D), BF16),
        ),
        in_specs=[hbm] * 4,
        out_specs=(hbm,) * 4,
        scratch_shapes=[
            pltpu.VMEM((B, T, H, D), BF16),
            pltpu.VMEM((B, T, H, D), BF16),
            pltpu.VMEM((TB * PITCH, D), F32),
            pltpu.VMEM((TB * PITCH, D), F32),
            pltpu.VMEM((2048, 2048), BF16),
            pltpu.VMEM((B, H, D, D), F32),
            pltpu.VMEM((B, H, D), F32),
            pltpu.VMEM((B, 2, 4, ROWS, D), BF16),
            pltpu.VMEM((B, 2, 3, ROWS, D), BF16),
            pltpu.VMEM((B, 2, ROWS, D), BF16),
            pltpu.VMEM((B, 2, 3, ROWS, D), BF16),
            pltpu.VMEM((B, 2, 4, ROWS, D), BF16),
            pltpu.VMEM((16, D), F32),
            pltpu.VMEM((B, H, T, D), BF16),
            pltpu.VMEM((T, 2048), BF16),
            pltpu.VMEM((4, 256, 256), BF16),
            pltpu.VMEM((D, D), F32),
            pltpu.VMEM((T, 2048), BF16),
            dma((2, 2 * B * NC)), dma((B,)), dma, dma((4,)), dma((4,)), dma((2,)),
            dma((2, 4)), dma((2, 4)), dma, dma, dma((3,)), dma((3,)), dma((2, 3)), dma((2, 3)),
            dma((11,)), dma((11,)),
            dma((4, 3)), dma((4, 3)), dma((4, 3)), dma((4, 3)), dma((4, 3)), dma((4, 3)),
        ],
        compiler_params=pltpu.CompilerParams(
            collective_id=0, has_side_effects=True, vmem_limit_bytes=63 * 2**20
        ),
        name="gather",
    )(q, k, v, w)


def finish_kernel(
    fq_hbm, st_hbm, w_hbm, first_hbm, o_hbm,
    fq, st, rhs, cols_of, mixed, wbuf, fbuf, obuf, q_sem, s_sem, w_sem, f_sem, o_sem,
):
    def get_q(n, g):
        hs = pl.ds(g * 8 + 2 * n, 2)
        return pltpu.make_async_copy(fq_hbm.at[hs], fq.at[hs], q_sem.at[n, g])

    def get_w(n):
        cols = pl.ds(n * TN, TN)
        return pltpu.make_async_copy(w_hbm.at[:, cols], wbuf.at[:, cols], w_sem.at[n])

    def put(n, i):
        rows, cols = pl.ds(i * (T // 2), T // 2), pl.ds(n * CN, CN)
        return pltpu.make_async_copy(obuf.at[rows, cols], o_hbm.at[1, rows, cols], o_sem.at[n, i])

    get_st = pltpu.make_async_copy(st_hbm, st, s_sem)
    get_st.start()
    for n in range(4):
        for g in range(2):
            get_q(n, g).start()
    get_first = pltpu.make_async_copy(first_hbm, fbuf, f_sem.at[0])
    put_first = pltpu.make_async_copy(fbuf, o_hbm.at[0], f_sem.at[1])
    cols_of[...] = jnp.zeros_like(cols_of)
    rhs[...] = jnp.zeros_like(rhs)
    get_st.wait()

    def step(n, _):
        for g in range(2):
            get_q(n, g).wait()
        get_w(n).start()
        look_up(fq, st, rhs, cols_of, mixed, (n, n))
        return 0

    lax.fori_loop(0, 4, step, 0)
    get_first.start()
    for n in range(2):
        get_w(2 * n).wait()
        get_w(2 * n + 1).wait()
        if n == 1:
            get_first.wait()
            put_first.start()
        cols = slice(n * CN, (n + 1) * CN)
        for i in range(2):
            rows = slice(i * (T // 2), (i + 1) * (T // 2))
            obuf[rows, cols] = jnp.dot(
                mixed[rows, :], wbuf[:, cols], preferred_element_type=F32
            ).astype(BF16)
            put(n, i).start()
    put_first.wait()
    for n in range(2):
        for i in range(2):
            put(n, i).wait()


def finish(fq1, st1, w, out0):
    dma = pltpu.SemaphoreType.DMA
    hbm = pl.BlockSpec(memory_space=pl.ANY)
    return pl.pallas_call(
        finish_kernel,
        in_specs=[hbm] * 4,
        out_specs=hbm,
        out_shape=jax.ShapeDtypeStruct((B, T, 2048), BF16),
        scratch_shapes=[
            pltpu.VMEM((H, T, D), BF16),
            pltpu.VMEM((2, 4, ROWS, D), BF16),
            pltpu.VMEM((4, 256, 256), BF16),
            pltpu.VMEM((D, D), F32),
            pltpu.VMEM((T, 2048), BF16),
            pltpu.VMEM((2048, 2048), BF16),
            pltpu.VMEM((T, 2048), BF16),
            pltpu.VMEM((T, 2048), BF16),
            dma((4, 2)), dma, dma((4,)), dma((2,)), dma((2, 2)),
        ],
        compiler_params=pltpu.CompilerParams(vmem_limit_bytes=60 * 2**20),
        name="finish",
    )(fq1, st1, w, out0)


def on_device(queries_in, keys_in, values_in, out_weight):
    w, out0, fq1, st1 = gather(queries_in, keys_in, values_in, out_weight)
    return finish(fq1, st1, w, out0)


def solution(mesh):
    placed = (
        P("dp", "sp", None, None),
        P("dp", "sp", None, None),
        P("dp", "sp", None, None),
        P("dp", None),
    )
    return jax.shard_map(
        on_device, mesh=mesh, in_specs=placed, out_specs=P("dp", "sp", None), check_vma=False
    )
```
